256 devices in a mesh: depth: 32 (over y, z_lo, core), chan: 8 (over x, z_hi).
Axes of the slice: x: 4, y: 4, z: 8 (z_hi: 2, z_lo: 4; z = z_hi * 4 + z_lo), core: 2. Of those that a mesh axis runs over, the one named last changes fastest.
Arguments:
- pre: float32 [1, 512, 64, 256], P(None, 'chan', 'depth'), may hold values from -6 to 6
- grad_out: float32 [1, 512, 64, 256], P(None, 'chan', 'depth'), may hold values from -6 to 6
- weight: float32 [27, 512, 512], P(None, 'chan'), may hold values from -0.0546875 to 0.0546875
Outputs:
- grad_pre: float32 [1, 512, 64, 256], P(None, 'chan', 'depth')
- grad_weight: float32 [27, 512, 512], P(None, 'chan', 'depth')
The draws below stay inside these ranges and needn't reach their ends.
All inputs are finite; a program needn't handle non-finite values.
Results may differ from the reference program's by a relative error of at most 0.0001.
Values sent between devices are 32-bit elements; how exact they have to be, the bound alone decides.
No kernel may reach another device: no remote copies, remote signals or barrier semaphores. Data moves between devices by JAX's collectives and lax.ppermute only.
A program may use at most 192 MiB of HBM per device.

```python
import math
import jax
import jax.numpy as jnp
from jax import lax

C = 512
W = 16
BATCH = 1
PLANE = 256
DEPTH = 64
VOXELS = 16384


def strengthened(result, stream_key, source, target, blocks, factor):
    owner, partner = [(jnp.arange(result.shape[position]) // (result.shape[position] // blocks)).reshape([-1 if axis == position else 1 for axis in range(result.ndim)]) for position in (source, target)]
    chosen = jax.random.permutation(stream_key, blocks)[partner]
    strong = (owner == chosen) | (owner == (partner + blocks // 2) % blocks)
    return jnp.where(strong, factor * result, result)


def shard_levels(stream_key, dims, shards, low, top_value):
    level, own = 1.0, jax.random.fold_in(stream_key, 6)
    for dim, blocks in shards:
        draws = jnp.exp(jax.random.uniform(jax.random.fold_in(own, dim), (blocks,), jnp.float32, low / len(shards), top_value / len(shards)))
        level = level * jnp.repeat(draws, dims[dim] // blocks).reshape([-1 if axis == dim else 1 for axis in range(len(dims))])
    return level


def normal_values(stream_key, extent, width, reach, split=(), kind=jnp.bfloat16):
    drawn = width * jax.random.normal(stream_key, extent, jnp.float32)
    if split:
        drawn = drawn * shard_levels(stream_key, extent, split, -0.22, 0.18)
    return jnp.clip(drawn, -reach, reach).astype(kind)


def gaussian_with(own_key, extent, deviation, reach, pieces, heavy, dtype=jnp.bfloat16):
    entries = deviation * jax.random.normal(own_key, extent, jnp.float32)
    if pieces:
        entries = entries * shard_levels(own_key, extent, pieces, -0.22, 0.18)
    return jnp.clip(strengthened(entries, jax.random.fold_in(own_key, 3), *heavy), -reach, reach).astype(dtype)


def setup_inputs(seed: int = 0) -> dict:
    arg_keys = jax.random.split(jax.random.key(seed), 4)
    pre = normal_values(arg_keys[0], (BATCH, C, DEPTH, PLANE), 1.0, 6.0, ((1, 8), (2, 32)), jnp.float32)
    grad_out = gaussian_with(arg_keys[1], (BATCH, C, DEPTH, PLANE), 1.0, 6.0, ((1, 8), (2, 32)), (2, 1, 32, 2.75), jnp.float32)
    weight = normal_values(arg_keys[2], (27, C, C), (27 * C) ** -0.5, 0.0546875, ((1, 8),), jnp.float32)
    return {"pre": pre, "grad_out": grad_out, "weight": weight}


def shift_plane(block, drow, dcol):
    plane = block.shape[-1]
    step = drow * W + dcol
    lead = [(0, 0)] * (block.ndim - 1)
    if step > 0:
        moved = jnp.pad(block[..., step:], lead + [(0, step)])
    elif step < 0:
        moved = jnp.pad(block[..., :plane + step], lead + [(-step, 0)])
    else:
        moved = block
    column = jnp.arange(plane) % W
    valid = (column + dcol >= 0) & (column + dcol < W)
    return jnp.where(valid, moved, jnp.float32(0.0))

def normal_cdf(value):
    return 0.5 * (1.0 + jax.scipy.special.erf(value / math.sqrt(2.0)))

def reference(pre, grad_out, weight):
    act = pre * normal_cdf(pre)
    depth_pad = [(0, 0), (0, 0), (1, 1), (0, 0)]
    act_pad = jnp.pad(act, depth_pad)
    cot_pad = jnp.pad(grad_out, depth_pad)
    grad_act = jnp.zeros(pre.shape, jnp.float32)
    filters = []
    for depth_off in range(3):
        for row_off in range(3):
            for col_off in range(3):
                index = 9 * depth_off + 3 * row_off + col_off
                source = shift_plane(act_pad[:, :, depth_off:depth_off + DEPTH], row_off - 1, col_off - 1)
                filters.append(jnp.einsum('bcdp,bodp->co', source, grad_out, precision=lax.Precision.HIGHEST))
                moved = shift_plane(cot_pad[:, :, 2 - depth_off:2 - depth_off + DEPTH], 1 - row_off, 1 - col_off)
                grad_act = grad_act + jnp.einsum('co,bodp->bcdp', weight[index], moved, precision=lax.Precision.HIGHEST)
    slope = normal_cdf(pre) + pre * jnp.exp(-0.5 * pre * pre) / math.sqrt(2.0 * math.pi)
    grad_pre = grad_act * slope
    grad_weight = jnp.stack(filters) * float(VOXELS) ** (-0.5)
    return (grad_pre, grad_weight)
```

```python
import math

import jax
import jax.numpy as jnp
from jax import lax
from jax.experimental import pallas as pl
from jax.experimental.pallas import tpu as pltpu
from jax.sharding import Mesh, PartitionSpec as P


W = 16
CELLS = 256
TAPS = 576
LANES = 1792
GRANT = 24 * 1024 * 1024
DEPTH_AXES = ("y", "zl", "core")
NT = (((1,), (1,)), ((), ()))
NN = (((1,), (0,)), ((), ()))


def normal_cdf(value):
    return 0.5 * (1.0 + jax.scipy.special.erf(value / math.sqrt(2.0)))


def split(value):
    hi = value.astype(jnp.bfloat16)
    lo = (value - hi.astype(jnp.float32)).astype(jnp.bfloat16)
    return hi, lo


def mul(a, b, dims):
    return lax.dot_general(a, b, dims, preferred_element_type=jnp.float32)


def moved(block, step):
    return block if step == 0 else pltpu.roll(block, (-step) % CELLS, 1)


def col_ok(shape, dcol):
    column = lax.broadcasted_iota(jnp.int32, shape, 1) % W
    return (column + dcol >= 0) & (column + dcol < W)


def row_ok(shape, drow):
    row = lax.broadcasted_iota(jnp.int32, shape, 1) // W
    return (row + drow >= 0) & (row + drow < CELLS // W)


def shift_cols(block, dcol):
    if dcol == 0:
        return block
    return jnp.where(col_ok(block.shape, dcol), moved(block, dcol), 0.0)


def shift_rows(block, drow):
    if drow == 0:
        return block
    return jnp.where(row_ok(block.shape, drow), moved(block, drow * W), 0.0)


def call(kernel, out_shapes, n_in, scratch=(), flops=0, moved_bytes=0):
    vmem = pl.BlockSpec(memory_space=pltpu.VMEM)
    return pl.pallas_call(
        kernel,
        out_shape=out_shapes,
        in_specs=[pl.BlockSpec(memory_space=pltpu.SMEM)] + [vmem] * n_in,
        out_specs=jax.tree.map(lambda _: vmem, out_shapes),
        scratch_shapes=scratch,
        cost_estimate=pl.CostEstimate(flops=flops, bytes_accessed=moved_bytes, transcendentals=0),
        compiler_params=pltpu.CompilerParams(vmem_limit_bytes=GRANT),
    )


def weight_kernel(ids, w_ref, hi_ref, lo_ref):
    core = ids[2]
    even = (lax.broadcasted_iota(jnp.int32, (64, 128), 1) // 16) % 2 == 0

    def tap_body(tap, carry):
        rows = pl.ds(pl.multiple_of(64 * tap, 64), 64)
        for kd in range(3):
            for pair in range(2):
                first = w_ref[9 * kd + tap, :, 256 * pair : 256 * pair + 128]
                second = w_ref[9 * kd + tap, :, 256 * pair + 128 : 256 * pair + 256]
                low = jnp.where(even, first, pltpu.roll(second, 16, 1))
                high = jnp.where(even, pltpu.roll(first, 112, 1), second)
                hi, lo = split(jnp.where(core == 0, low, high))
                lanes = slice(256 * kd + 128 * pair, 256 * kd + 128 * pair + 128)
                hi_ref[rows, lanes] = hi
                lo_ref[rows, lanes] = lo
        return carry

    lax.fori_loop(0, 9, tap_body, 0)


def pick_weights(ids, weight):
    shape = jax.ShapeDtypeStruct((TAPS, 3 * CELLS), jnp.bfloat16)
    return call(weight_kernel, (shape, shape), 1, flops=200000000, moved_bytes=5000000)(ids, weight)


def act_kernel(ids, own, sib, edge, far_edge, hi_ref, lo_ref):
    core = ids[2]
    planes = [
        (own[0], 1 + 2 * core),
        (own[1], 2 + 2 * core),
        (sib[0], 3 - 2 * core),
        (sib[1], 4 - 2 * core),
        (edge[...], 5 * core),
        (far_edge[...], 5 - 5 * core),
    ]
    for block, place in planes:
        for dcol in (-1, 0, 1):
            cols = shift_cols(block, dcol)
            for drow in (-1, 0, 1):
                hi, lo = split(shift_rows(cols, drow))
                tap = 3 * (drow + 1) + dcol + 1
                rows = pl.ds(pl.multiple_of(TAPS * place + 64 * tap, 64), 64)
                hi_ref[rows, :] = hi
                lo_ref[rows, :] = lo
    hi_ref[6 * TAPS :, :] = jnp.zeros((64, CELLS), jnp.bfloat16)
    lo_ref[6 * TAPS :, :] = jnp.zeros((64, CELLS), jnp.bfloat16)


def expand_act(ids, own, sib, edge, far_edge):
    shape = jax.ShapeDtypeStruct((6 * TAPS + 64, CELLS), jnp.bfloat16)
    return call(act_kernel, (shape, shape), 4, flops=50000000, moved_bytes=4000000)(
        ids, own, sib, edge, far_edge
    )


def filter_kernel(ids, b0, b1, b2, b3, ahi, alo, o0, o1, o2, o3, both):
    y, core, x = ids[0], ids[2], ids[3]
    for s, block in enumerate((b0, b1, b2, b3)):
        u = (x - s - y + 8) % 4
        rows = pl.ds(pl.multiple_of(32 * u, 32), 32)
        rows_lo = pl.ds(pl.multiple_of(128 + 32 * u, 32), 32)
        for j in range(4):
            q = (j + 2 * core) % 4
            hi, lo = split(block[j])
            both[q, rows, :] = hi
            both[q, rows_lo, :] = lo
    outs = (o0, o1, o2, o3)
    for n in range(LANES // 256):
        wide = jnp.zeros((256, 256), jnp.float32)
        narrow = jnp.zeros((128, 256), jnp.float32)
        for q in range(4):
            taps = slice(TAPS * q + 256 * n, TAPS * q + 256 * n + 256)
            wide += mul(both[q], ahi[taps, :], NT)
            narrow += mul(both[q, :128], alo[taps, :], NT)
        total = wide[:128] + wide[128:] + narrow
        for u in range(4):
            outs[u][:, 256 * n : 256 * n + 256] = total[32 * u : 32 * u + 32]


def filter_terms(ids, blocks, ahi, alo):
    shape = jax.ShapeDtypeStruct((32, LANES), jnp.float32)
    scratch = [pltpu.VMEM((4, 256, CELLS), jnp.bfloat16)]
    return call(
        filter_kernel, (shape,) * 4, 6, scratch, flops=1400000000, moved_bytes=5000000
    )(ids, *blocks, ahi, alo)


def grad_kernel(ids, *refs):
    blocks, (whi, wlo, keep, send, ghi, glo) = refs[:8], refs[8:]
    core, x, zh = ids[2], ids[3], ids[4]
    for n, block in enumerate(blocks):
        src_x = (x - n % 4 + 4) % 4
        src_zh = zh if n < 4 else 1 - zh
        base = 128 * (src_x // 2) + 64 * src_zh + 16 * (src_x % 2)
        for j in range(4):
            q = (j + 2 * core) % 4
            hi, lo = split(block[j])
            for b in range(2):
                rows = pl.ds(pl.multiple_of((3 - q) * 256 + base + 32 * b, 16), 16)
                ghi[rows, :] = hi[16 * b : 16 * b + 16]
                glo[rows, :] = lo[16 * b : 16 * b + 16]
    for p in range(6):
        first, last = max(0, p - 3), min(2, p)
        lanes = slice(256 * first, 256 * (last + 1))
        top = 256 * (3 - p + first)
        depth = slice(top, top + 256 * (last + 1 - first))
        total = None
        for kh in range(3):
            taps = slice(192 * kh, 192 * kh + 192)
            z = (
                mul(whi[taps, lanes], ghi[depth, :], NN)
                + mul(wlo[taps, lanes], ghi[depth, :], NN)
                + mul(whi[taps, lanes], glo[depth, :], NN)
            )
            part = (
                shift_cols(z[:64], 1) + z[64:128] + shift_cols(z[128:], -1)
            )
            part = shift_rows(part, 1 - kh)
            total = part if total is None else total + part
        m = min(p, 5 - p)
        mine = core == (1 if p >= 3 else 0)

        @pl.when(mine)
        def _():
            keep[m] = total

        @pl.when(jnp.logical_not(mine))
        def _():
            send[m] = total


def grad_terms(ids, blocks, whi, wlo):
    shape = jax.ShapeDtypeStruct((3, 64, CELLS), jnp.float32)
    scratch = [pltpu.VMEM((4 * 256, CELLS), jnp.bfloat16)] * 2
    return call(
        grad_kernel, (shape, shape), 10, scratch, flops=2800000000, moved_bytes=4000000
    )(ids, *blocks, whi, wlo)


def ring(n, step):
    return [(i, (i + step) % n) for i in range(n)]


def work(pre, grad_out, weight):
    y, zl, core, x, zh = [lax.axis_index(a) for a in ("y", "zl", "core", "x", "zh")]
    ids = jnp.stack([y, zl, core, x, zh]).astype(jnp.int32)
    swap = [(0, 1), (1, 0)]

    cot = jnp.moveaxis(grad_out[0], 1, 0).reshape(2, 2, 2, 16, CELLS)
    mine = lax.dynamic_index_in_dim(cot, core, 2, keepdims=False).reshape(2, 32, CELLS)
    theirs = lax.dynamic_index_in_dim(cot, 1 - core, 2, keepdims=False).reshape(2, 32, CELLS)
    cot4 = jnp.concatenate([mine, lax.ppermute(theirs, "core", swap)], axis=0)
    across = lax.ppermute(cot4, "zh", swap)
    near = [cot4] + [lax.ppermute(cot4, "x", ring(4, s)) for s in (1, 2, 3)]
    far = [across] + [lax.ppermute(across, "x", ring(4, s)) for s in (1, 2, 3)]

    source = jnp.moveaxis(pre[0], 1, 0)
    cdf = normal_cdf(source)
    slope = cdf + source * jnp.exp(-0.5 * source * source) / math.sqrt(2.0 * math.pi)
    act, slope = lax.optimization_barrier((source * cdf, slope))
    edge = lax.dynamic_index_in_dim(act, core, 0, keepdims=False)
    outward = []
    for chip in range(16):
        if chip < 15:
            outward.append((2 * chip + 1, 2 * chip + 2))
        if chip > 0:
            outward.append((2 * chip, 2 * chip - 1))
    sib = lax.ppermute(act, "core", swap)
    edge = lax.ppermute(edge, DEPTH_AXES, outward)
    far_edge = lax.ppermute(edge, "core", swap)

    whi, wlo = pick_weights(ids, weight)
    ahi, alo = expand_act(ids, act, sib, edge, far_edge)

    def over_y(parts):
        total = parts[0]
        for t in (1, 2, 3):
            total = total + lax.ppermute(parts[t], "y", ring(4, t))
        return total

    sum_near = over_y(filter_terms(ids, near, ahi, alo))
    sum_far = over_y(filter_terms(ids, far, ahi, alo))
    keep, send = grad_terms(ids, near + far, whi, wlo)

    both = jnp.stack([sum_near, sum_far]).reshape(4, 16, LANES)

    def part_for(t):
        z = (zl + t) % 4
        return lax.dynamic_index_in_dim(both, 2 * ((z // 2 + zh) % 2) + z % 2, 0, keepdims=False)

    total = part_for(0)
    for t in (1, 2, 3):
        total = total + lax.ppermute(part_for(t), "zl", ring(4, t))
    total = total * float(16384) ** (-0.5)
    grad_weight = total.reshape(16, 28, 64)[:, :27].transpose(1, 2, 0)

    got = keep + lax.ppermute(send, "core", swap)
    close = got[1] + lax.ppermute(got[0], DEPTH_AXES, outward)
    grad_act = jnp.where(core == 0, jnp.stack([close, got[2]]), jnp.stack([got[2], close]))
    grad_pre = jnp.moveaxis(grad_act * slope, 0, 1)[None]
    return (grad_pre, grad_weight)


def solution(mesh):
    fine = Mesh(mesh.devices.reshape(4, 4, 2, 4, 2), ("y", "zl", "core", "x", "zh"))
    chan, depth = ("x", "zh"), DEPTH_AXES
    return jax.shard_map(
        work,
        mesh=fine,
        in_specs=(P(None, chan, depth, None), P(None, chan, depth, None), P(None, chan, None)),
        out_specs=(P(None, chan, depth, None), P(None, chan, depth)),
        check_vma=False,
    )
```

```python
import math

import jax
import jax.numpy as jnp
from jax import lax
from jax.experimental import pallas as pl
from jax.experimental.pallas import tpu as pltpu
from jax.sharding import Mesh, PartitionSpec as P


W = 16
CELLS = 256
TAPS = 576
LANES = 1792
GRANT = 24 * 1024 * 1024
DEPTH_AXES = ("y", "zl", "core")
NT = (((1,), (1,)), ((), ()))
NN = (((1,), (0,)), ((), ()))


def normal_cdf(value):
    return 0.5 * (1.0 + jax.scipy.special.erf(value / math.sqrt(2.0)))


def split(value):
    hi = value.astype(jnp.bfloat16)
    lo = (value - hi.astype(jnp.float32)).astype(jnp.bfloat16)
    return hi, lo


def mul(a, b, dims):
    return lax.dot_general(a, b, dims, preferred_element_type=jnp.float32)


def moved(block, step):
    return block if step == 0 else pltpu.roll(block, (-step) % CELLS, 1)


def col_ok(shape, dcol):
    column = lax.broadcasted_iota(jnp.int32, shape, 1) % W
    return (column + dcol >= 0) & (column + dcol < W)


def row_ok(shape, drow):
    row = lax.broadcasted_iota(jnp.int32, shape, 1) // W
    return (row + drow >= 0) & (row + drow < CELLS // W)


def shift_cols(block, dcol):
    if dcol == 0:
        return block
    return jnp.where(col_ok(block.shape, dcol), moved(block, dcol), 0.0)


def shift_rows(block, drow):
    if drow == 0:
        return block
    return jnp.where(row_ok(block.shape, drow), moved(block, drow * W), 0.0)


def call(kernel, out_shapes, n_in, scratch=(), flops=0, moved_bytes=0):
    vmem = pl.BlockSpec(memory_space=pltpu.VMEM)
    return pl.pallas_call(
        kernel,
        out_shape=out_shapes,
        in_specs=[pl.BlockSpec(memory_space=pltpu.SMEM)] + [vmem] * n_in,
        out_specs=jax.tree.map(lambda _: vmem, out_shapes),
        scratch_shapes=scratch,
        cost_estimate=pl.CostEstimate(flops=flops, bytes_accessed=moved_bytes, transcendentals=0),
        compiler_params=pltpu.CompilerParams(vmem_limit_bytes=GRANT),
    )


def weight_kernel(ids, w_ref, out_ref):
    place = 2 * ids[1] + ids[2]
    group = (lax.broadcasted_iota(jnp.int32, (64, 128), 1) // 16) % 4

    def tap_body(tap, carry):
        rows = pl.ds(pl.multiple_of(64 * tap, 64), 64)
        for kd in range(3):
            picked = jnp.zeros((64, 128), jnp.float32)
            for src in range(4):
                lanes = w_ref[9 * kd + tap, :, 128 * src : 128 * src + 128]
                turned = pltpu.roll(lanes, (16 * (src - place) + 128) % 128, 1)
                picked = jnp.where(group == src, turned, picked)
            hi, lo = split(picked)
            out_ref[rows, 128 * kd : 128 * kd + 128] = hi
            out_ref[rows, 384 + 128 * kd : 384 + 128 * kd + 128] = lo
        return carry

    lax.fori_loop(0, 9, tap_body, 0)


def pick_weights(ids, weight):
    shape = jax.ShapeDtypeStruct((TAPS, 768), jnp.bfloat16)
    return call(weight_kernel, shape, 1, flops=200000000, moved_bytes=5000000)(ids, weight)


def act_kernel(ids, own, sib, pair, cross, before, after, hi_ref, lo_ref):
    base = 4 * ids[1] + 2 * ids[2]
    planes = [(before[...], 0), (after[...], 9)]
    for n, block in enumerate((own, sib, pair, cross)):
        planes += [(block[j], (base ^ (2 * n)) + 1 + j) for j in range(2)]
    for block, place in planes:
        for dcol in (-1, 0, 1):
            cols = shift_cols(block, dcol)
            for drow in (-1, 0, 1):
                hi, lo = split(shift_rows(cols, drow))
                tap = 3 * (drow + 1) + dcol + 1
                rows = pl.ds(pl.multiple_of(TAPS * place + 64 * tap, 64), 64)
                hi_ref[rows, :] = hi
                lo_ref[rows, :] = lo
    hi_ref[10 * TAPS :, :] = jnp.zeros((64, CELLS), jnp.bfloat16)
    lo_ref[10 * TAPS :, :] = jnp.zeros((64, CELLS), jnp.bfloat16)


def expand_act(ids, *planes):
    shape = jax.ShapeDtypeStruct((10 * TAPS + 64, CELLS), jnp.bfloat16)
    return call(act_kernel, (shape, shape), 6, flops=50000000, moved_bytes=4000000)(ids, *planes)


def filter_kernel(ids, *refs):
    blocks, (ahi, alo), outs, both = refs[:8], refs[8:10], refs[10:14], refs[14]
    y, x, base = ids[0], ids[3], 4 * ids[1] + 2 * ids[2]
    for n, block in enumerate(blocks):
        u = (x - n % 4 - y + 8) % 4
        row = 32 * u + 16 * (n // 4)
        for i in range(4):
            for j in range(2):
                q = (base ^ (2 * i)) + j
                hi, lo = split(block[2 * i + j])
                both[q, pl.ds(pl.multiple_of(row, 16), 16), :] = hi
                both[q, pl.ds(pl.multiple_of(row + 128, 16), 16), :] = lo
    for n in range(LANES // 256):
        wide = jnp.zeros((256, 256), jnp.float32)
        narrow = jnp.zeros((128, 256), jnp.float32)
        for q in range(8):
            taps = slice(TAPS * q + 256 * n, TAPS * q + 256 * n + 256)
            wide += mul(both[q], ahi[taps, :], NT)
            narrow += mul(both[q, :128], alo[taps, :], NT)
        total = wide[:128] + wide[128:] + narrow
        for u in range(4):
            outs[u][:, 256 * n : 256 * n + 256] = total[32 * u : 32 * u + 32]


def filter_terms(ids, blocks, ahi, alo):
    shape = jax.ShapeDtypeStruct((32, LANES), jnp.float32)
    scratch = [pltpu.VMEM((8, 256, CELLS), jnp.bfloat16)]
    return call(
        filter_kernel, (shape,) * 4, 10, scratch, flops=2800000000, moved_bytes=9000000
    )(ids, *blocks, ahi, alo)


KEPT = (0, 1, 2, 5, 6)


def grad_kernel(ids, *refs):
    blocks, (w_ref, keep, send, ghi, glo) = refs[:8], refs[8:]
    core, x, zh, base = ids[2], ids[3], ids[4], 4 * ids[1] + 2 * ids[2]
    for n, block in enumerate(blocks):
        src_x = (x - n % 4 + 4) % 4
        src_zh = zh if n < 4 else 1 - zh
        place = 64 * src_zh + 16 * src_x
        for i in range(4):
            for j in range(2):
                q = (base ^ (2 * i)) + j
                hi, lo = split(block[2 * i + j])
                rows = pl.ds(pl.multiple_of((7 - q) * 128 + place, 16), 16)
                ghi[rows, :] = hi
                glo[rows, :] = lo
    for p in range(10):
        first, last = max(0, p - 7), min(2, p)
        whi = w_ref[:, 128 * first : 128 * (last + 1)]
        wlo = w_ref[:, 384 + 128 * first : 384 + 128 * (last + 1)]
        top = 128 * (7 - p + first)
        depth = slice(top, top + 128 * (last + 1 - first))
        z = mul(
            jnp.concatenate([whi, wlo, whi], axis=1),
            jnp.concatenate([ghi[depth, :], ghi[depth, :], glo[depth, :]], axis=0),
            NN,
        )
        total = None
        for kh in range(3):
            rows = z[192 * kh : 192 * kh + 192]
            part = shift_cols(rows[:64], 1) + rows[64:128] + shift_cols(rows[128:], -1)
            part = shift_rows(part, 1 - kh)
            total = part if total is None else total + part
        kept_by_first = p in KEPT
        m = KEPT.index(p if kept_by_first else 9 - p)
        mine = core == (0 if kept_by_first else 1)

        @pl.when(mine)
        def _():
            keep[m] = total

        @pl.when(jnp.logical_not(mine))
        def _():
            send[m] = total


def grad_terms(ids, blocks, weights):
    shape = jax.ShapeDtypeStruct((5, 64, CELLS), jnp.float32)
    scratch = [pltpu.VMEM((8 * 128, CELLS), jnp.bfloat16)] * 2
    return call(
        grad_kernel, (shape, shape), 9, scratch, flops=2800000000, moved_bytes=4000000
    )(ids, *blocks, weights)


def ring(n, step):
    return [(i, (i + step) % n) for i in range(n)]


def sent(x, axis, pairs):
    return lax.ppermute(x, axis, pairs)


def pick(x, index, axis=0):
    return lax.dynamic_index_in_dim(x, index, axis, keepdims=False)


def work(pre, grad_out, weight):
    y, zl, core, x, zh = [lax.axis_index(a) for a in ("y", "zl", "core", "x", "zh")]
    side, half = zl % 2, zl // 2
    ids = jnp.stack([y, side, core, x, zh]).astype(jnp.int32)
    swap = [(0, 1), (1, 0)]
    pair_swap = [(i, i ^ 1) for i in range(4)]
    half_swap = [(i, i ^ 2) for i in range(4)]
    outward = [(4 * n + 3, 4 * n + 4) for n in range(7)] + [(4 * n + 4, 4 * n + 3) for n in range(7)]

    cot = jnp.moveaxis(grad_out[0], 1, 0).reshape(2, 2, 2, 16, CELLS)
    theirs = sent(pick(cot, 1 - core, 2), "core", swap)
    chip = jnp.stack([pick(cot, core, 2), theirs]).reshape(4, 2, 16, CELLS)
    theirs = sent(pick(chip, 1 - side, 1), "zl", pair_swap)
    cot8 = jnp.concatenate([pick(chip, side, 1), theirs], axis=0)
    across = sent(cot8, "zh", swap)
    blocks = [cot8] + [sent(cot8, "x", ring(4, s)) for s in (1, 2, 3)]
    blocks += [across] + [sent(across, "x", ring(4, s)) for s in (1, 2, 3)]

    source = jnp.moveaxis(pre[0], 1, 0)
    cdf = normal_cdf(source)
    slope = cdf + source * jnp.exp(-0.5 * source * source) / math.sqrt(2.0 * math.pi)
    own, slope = lax.optimization_barrier((source * cdf, slope))
    pair = sent(own, "zl", pair_swap)
    sib = sent(own, "core", swap)
    cross = sent(pair, "core", swap)
    place = 2 * side + core
    top = jnp.where(
        place < 2,
        jnp.where(place == 0, cross[1], pair[1]),
        jnp.where(place == 2, sib[1], own[1]),
    )
    bottom = jnp.where(
        place < 2,
        jnp.where(place == 0, own[0], sib[0]),
        jnp.where(place == 2, pair[0], cross[0]),
    )
    before = sent(top, DEPTH_AXES, [(d, d + 4) for d in range(28)])
    after = sent(bottom, DEPTH_AXES, [(d + 4, d) for d in range(28)])

    weights = pick_weights(ids, weight)
    ahi, alo = expand_act(ids, own, sib, pair, cross, before, after)

    parts = filter_terms(ids, blocks, ahi, alo)
    total = parts[0]
    for t in (1, 2, 3):
        total = total + sent(parts[t], "y", ring(4, t))
    total = total.reshape(2, 16, LANES)
    kept = pick(total, (half + zh) % 2)
    total = kept + sent(pick(total, (half + zh + 1) % 2), "zl", half_swap)
    total = total * float(16384) ** (-0.5)
    grad_weight = total.reshape(16, 28, 64)[:, :27].transpose(1, 2, 0)

    keep, send = grad_terms(ids, blocks, weights)
    got = keep + sent(send, "core", swap)
    outer, inner = got[:3], jnp.concatenate([got[:1], got[3:]], axis=0)
    edge = side == core
    got = jnp.where(edge, outer, inner) + sent(jnp.where(edge, inner, outer), "zl", pair_swap)
    close = got[1] + sent(got[0], DEPTH_AXES, outward)
    grad_act = jnp.where(core == 0, jnp.stack([close, got[2]]), jnp.stack([got[2], close]))
    grad_pre = jnp.moveaxis(grad_act * slope, 0, 1)[None]
    return (grad_pre, grad_weight)


def solution(mesh):
    fine = Mesh(mesh.devices.reshape(4, 4, 2, 4, 2), ("y", "zl", "core", "x", "zh"))
    chan, depth = ("x", "zh"), DEPTH_AXES
    return jax.shard_map(
        work,
        mesh=fine,
        in_specs=(P(None, chan, depth, None), P(None, chan, depth, None), P(None, chan, None)),
        out_specs=(P(None, chan, depth, None), P(None, chan, depth)),
        check_vma=False,
    )
```

```python
import math

import jax
import jax.numpy as jnp
from jax import lax
from jax.experimental import pallas as pl
from jax.experimental.pallas import tpu as pltpu
from jax.sharding import Mesh, PartitionSpec as P


W = 16
CELLS = 256
TAPS = 576
LANES = 1792
GRANT = 24 * 1024 * 1024
DEPTH_AXES = ("y", "zl", "core")
NT = (((1,), (1,)), ((), ()))
NN = (((1,), (0,)), ((), ()))


def normal_cdf(value):
    return 0.5 * (1.0 + jax.scipy.special.erf(value / math.sqrt(2.0)))


def split(value):
    hi = value.astype(jnp.bfloat16)
    lo = (value - hi.astype(jnp.float32)).astype(jnp.bfloat16)
    return hi, lo


def mul(a, b, dims):
    return lax.dot_general(a, b, dims, preferred_element_type=jnp.float32)


def moved(block, step):
    return block if step == 0 else pltpu.roll(block, (-step) % CELLS, 1)


def col_ok(shape, dcol):
    column = lax.broadcasted_iota(jnp.int32, shape, 1) % W
    return (column + dcol >= 0) & (column + dcol < W)


def row_ok(shape, drow):
    row = lax.broadcasted_iota(jnp.int32, shape, 1) // W
    return (row + drow >= 0) & (row + drow < CELLS // W)


def shift_cols(block, dcol):
    if dcol == 0:
        return block
    return jnp.where(col_ok(block.shape, dcol), moved(block, dcol), 0.0)


def shift_rows(block, drow):
    if drow == 0:
        return block
    return jnp.where(row_ok(block.shape, drow), moved(block, drow * W), 0.0)


def call(kernel, out_shapes, n_in, scratch=(), flops=0, moved_bytes=0):
    vmem = pl.BlockSpec(memory_space=pltpu.VMEM)
    return pl.pallas_call(
        kernel,
        out_shape=out_shapes,
        in_specs=[pl.BlockSpec(memory_space=pltpu.SMEM)] + [vmem] * n_in,
        out_specs=jax.tree.map(lambda _: vmem, out_shapes),
        scratch_shapes=scratch,
        cost_estimate=pl.CostEstimate(flops=flops, bytes_accessed=moved_bytes, transcendentals=0),
        compiler_params=pltpu.CompilerParams(vmem_limit_bytes=GRANT),
    )


def weight_kernel(ids, w_ref, out_ref):
    place = 2 * ids[1] + ids[2]
    group = (lax.broadcasted_iota(jnp.int32, (64, 128), 1) // 16) % 4

    def tap_body(tap, carry):
        rows = pl.ds(pl.multiple_of(64 * tap, 64), 64)
        for kd in range(3):
            picked = jnp.zeros((64, 128), jnp.float32)
            for src in range(4):
                lanes = w_ref[9 * kd + tap, :, 128 * src : 128 * src + 128]
                turned = pltpu.roll(lanes, (16 * (src - place) + 128) % 128, 1)
                picked = jnp.where(group == src, turned, picked)
            for part, value in enumerate(split(picked) * 2):
                if part < 3:
                    out_ref[rows, 384 * part + 128 * kd : 384 * part + 128 * kd + 128] = value
        return carry

    lax.fori_loop(0, 9, tap_body, 0)


def pick_weights(ids, weight):
    shape = jax.ShapeDtypeStruct((TAPS, 1152), jnp.bfloat16)
    return call(weight_kernel, shape, 1, flops=200000000, moved_bytes=5000000)(
        ids, weight
    )


def put_taps(block, start, hi_ref, lo_ref):
    for dcol in (-1, 0, 1):
        cols = shift_cols(block, dcol)
        for drow in (-1, 0, 1):
            hi, lo = split(shift_rows(cols, drow))
            tap = 3 * (drow + 1) + dcol + 1
            rows = pl.ds(pl.multiple_of(start + 64 * tap, 64), 64)
            hi_ref[rows, :] = hi
            lo_ref[rows, :] = lo


def chip_act_kernel(ids, own, sib, hi_ref, lo_ref):
    for n, duo in enumerate((own, sib)):
        for j in range(2):
            put_taps(duo[j], TAPS * (2 * n + j), hi_ref, lo_ref)


def pair_act_kernel(ids, edge, rim, pair, cross, hi_in, lo_in, hi_ref, lo_ref):
    base = 4 * ids[1] + 2 * ids[2]
    before = after = jnp.zeros((64, CELLS), jnp.float32)
    for n, outer in enumerate((edge[...], rim[...], pair[2], cross[2])):
        before = jnp.where(base ^ (2 * n) == 0, outer, before)
        after = jnp.where(base ^ (2 * n) == 6, outer, after)
    for n in range(2):
        start = pl.multiple_of(TAPS * ((base ^ (2 * n)) + 1), 64)
        rows = slice(2 * TAPS * n, 2 * TAPS * (n + 1))
        hi_ref[pl.ds(start, 2 * TAPS), :] = hi_in[rows, :]
        lo_ref[pl.ds(start, 2 * TAPS), :] = lo_in[rows, :]
    for n, trio in ((2, pair), (3, cross)):
        for j in range(2):
            put_taps(trio[j], TAPS * ((base ^ (2 * n)) + 1 + j), hi_ref, lo_ref)
    put_taps(before, 0, hi_ref, lo_ref)
    put_taps(after, 9 * TAPS, hi_ref, lo_ref)
    hi_ref[10 * TAPS :, :] = jnp.zeros((64, CELLS), jnp.bfloat16)
    lo_ref[10 * TAPS :, :] = jnp.zeros((64, CELLS), jnp.bfloat16)


def chip_act(ids, own, sib):
    shape = jax.ShapeDtypeStruct((4 * TAPS, CELLS), jnp.bfloat16)
    return call(chip_act_kernel, (shape, shape), 2, flops=2800000000, moved_bytes=9000000)(ids, own, sib)


def pair_act(ids, edge, rim, pair, cross, hi, lo):
    shape = jax.ShapeDtypeStruct((10 * TAPS + 64, CELLS), jnp.bfloat16)
    return call(pair_act_kernel, (shape, shape), 6, flops=30000000, moved_bytes=4000000)(
        ids, edge, rim, pair, cross, hi, lo
    )


def filter_kernel(ids, *refs):
    blocks, (ahi, alo), outs, both = refs[:8], refs[8:10], refs[10:14], refs[14]
    y, x, base = ids[0], ids[3], 4 * ids[1] + 2 * ids[2]
    for n, block in enumerate(blocks):
        u = (x - n % 4 - y + 8) % 4
        row = 32 * u + 16 * (n // 4)
        for i in range(4):
            for j in range(2):
                q = (base ^ (2 * i)) + j
                hi, lo = split(block[2 * i + j])
                both[q, pl.ds(pl.multiple_of(row, 16), 16), :] = hi
                both[q, pl.ds(pl.multiple_of(row + 128, 16), 16), :] = lo
    for n in range(LANES // 256):
        wide = jnp.zeros((256, 256), jnp.float32)
        narrow = jnp.zeros((128, 256), jnp.float32)
        for q in range(8):
            taps = slice(TAPS * q + 256 * n, TAPS * q + 256 * n + 256)
            wide += mul(both[q], ahi[taps, :], NT)
            narrow += mul(both[q, :128], alo[taps, :], NT)
        total = wide[:128] + wide[128:] + narrow
        for u in range(4):
            outs[u][:, 256 * n : 256 * n + 256] = total[32 * u : 32 * u + 32]


def filter_terms(ids, blocks, ahi, alo):
    shape = jax.ShapeDtypeStruct((32, LANES), jnp.float32)
    scratch = [pltpu.VMEM((8, 256, CELLS), jnp.bfloat16)]
    return call(filter_kernel, (shape,) * 4, 10, scratch, flops=2800000000, moved_bytes=9000000)(ids, *blocks, ahi, alo)


KEPT = (0, 1, 2, 5, 6)


def grad_kernel(ids, *refs):
    blocks, (w_ref, keep, send, ghi, glo, out) = refs[:8], refs[8:]
    core, x, zh, base = ids[2], ids[3], ids[4], 4 * ids[1] + 2 * ids[2]
    for n, block in enumerate(blocks):
        src_x = (x - n % 4 + 4) % 4
        src_zh = zh if n < 4 else 1 - zh
        place = 64 * src_zh + 16 * src_x
        for i in range(4):
            for j in range(2):
                q = (base ^ (2 * i)) + j
                hi, lo = split(block[2 * i + j])
                rows = pl.ds(pl.multiple_of((7 - q) * 128 + place, 16), 16)
                ghi[rows, :] = hi
                glo[rows, :] = lo
    for p in range(10):
        first, last = max(0, p - 7), min(2, p)
        top = 128 * (7 - p + first)
        depth = slice(top, top + 128 * (last + 1 - first))
        if last - first == 2:
            lhs = w_ref[...]
        else:
            lhs = jnp.concatenate(
                [w_ref[:, 384 * n + 128 * first : 384 * n + 128 * (last + 1)] for n in range(3)], axis=1
            )
        z = mul(
            lhs,
            jnp.concatenate([ghi[depth, :], ghi[depth, :], glo[depth, :]], axis=0),
            NN,
        )
        total = None
        for kh in range(3):
            rows = z[192 * kh : 192 * kh + 192]
            part = shift_cols(rows[:64], 1) + rows[64:128] + shift_cols(rows[128:], -1)
            part = shift_rows(part, 1 - kh)
            total = part if total is None else total + part
        kept_by_first = p in KEPT
        m = KEPT.index(p if kept_by_first else 9 - p)
        out[core if kept_by_first else 1 - core, m] = total
    keep[...] = out[0]
    send[...] = out[1]


def grad_terms(ids, blocks, weights):
    shape = jax.ShapeDtypeStruct((5, 64, CELLS), jnp.float32)
    scratch = [pltpu.VMEM((8 * 128, CELLS), jnp.bfloat16)] * 2 + [pltpu.VMEM((2, 5, 64, CELLS), jnp.float32)]
    return call(grad_kernel, (shape, shape), 9, scratch, flops=2800000000, moved_bytes=4000000)(ids, *blocks, weights)


def ring(n, step):
    return [(i, (i + step) % n) for i in range(n)]


def sent(x, axis, pairs):
    return lax.ppermute(x, axis, pairs)


def pick(x, index, axis=0):
    return lax.dynamic_index_in_dim(x, index, axis, keepdims=False)


def work(pre, grad_out, weight):
    y, zl, core, x, zh = [lax.axis_index(a) for a in ("y", "zl", "core", "x", "zh")]
    side, half = zl % 2, zl // 2
    ids = jnp.stack([y, side, core, x, zh]).astype(jnp.int32)
    swap = [(0, 1), (1, 0)]
    pair_swap = [(i, i ^ 1) for i in range(4)]
    half_swap = [(i, i ^ 2) for i in range(4)]
    outward = [(4 * n + 3, 4 * n + 4) for n in range(7)] + [(4 * n + 4, 4 * n + 3) for n in range(7)]

    cot = jnp.moveaxis(grad_out[0], 1, 0).reshape(2, 2, 2, 16, CELLS)
    theirs = sent(pick(cot, 1 - core, 2), "core", swap)
    chip = jnp.stack([pick(cot, core, 2), theirs]).reshape(4, 2, 16, CELLS)
    ours, theirs = pick(chip, side, 1), pick(chip, 1 - side, 1)
    both_swap = [(2 * i + j, 2 * (i ^ 1) + 1 - j) for i in range(4) for j in range(2)]
    far_pair = sent(theirs, ("zl", "zh"), both_swap)
    across = jnp.concatenate([sent(ours, "zh", swap), far_pair], axis=0)
    cot8 = jnp.concatenate([ours, sent(theirs, "zl", pair_swap)], axis=0)
    blocks = [cot8] + [sent(cot8, "x", ring(4, s)) for s in (1, 2, 3)]
    blocks += [across] + [sent(across, "x", ring(4, s)) for s in (1, 2, 3)]

    source = jnp.moveaxis(pre[0], 1, 0)
    cdf = normal_cdf(source)
    slope = cdf + source * jnp.exp(-0.5 * source * source) / math.sqrt(2.0 * math.pi)
    own, slope = lax.optimization_barrier((source * cdf, slope))
    sib = sent(own, "core", swap)
    edge = sent(pick(own, core), DEPTH_AXES, outward)
    trio = jnp.concatenate([own, edge[None]], axis=0)
    pair = sent(trio, "zl", pair_swap)
    rim = sent(edge, "core", swap)
    cross = sent(pair, "core", swap)

    weights = pick_weights(ids, weight)
    ahi, alo = chip_act(ids, own, sib)
    ahi, alo = pair_act(ids, edge, rim, pair, cross, ahi, alo)

    parts = filter_terms(ids, blocks, ahi, alo)
    arrived = [sent(parts[t], "y", ring(4, t)) for t in (1, 2, 3)]
    total = parts[0] + arrived[0] + arrived[1] + arrived[2]
    total = total.reshape(2, 16, LANES)
    kept = pick(total, (half + zh) % 2)
    total = kept + sent(pick(total, (half + zh + 1) % 2), "zl", half_swap)
    total = total * float(16384) ** (-0.5)
    grad_weight = total.reshape(16, 28, 64)[:, :27].transpose(1, 2, 0)

    keep, send = grad_terms(ids, blocks, weights)
    got = keep + sent(send, "core", swap)
    outer, inner = got[1:3], got[3:]
    edge = side == core
    fringe = sent(got[0], DEPTH_AXES, outward)
    crossing = [(4 * n + 1, 4 * n + 4) for n in range(7)] + [(4 * n + 6, 4 * n + 3) for n in range(7)]
    fringe = fringe + sent(got[0], DEPTH_AXES, crossing)
    got = jnp.where(edge, outer, inner) + sent(jnp.where(edge, inner, outer), "zl", pair_swap)
    close = got[0] + fringe
    grad_act = jnp.where(core == 0, jnp.stack([close, got[1]]), jnp.stack([got[1], close]))
    grad_pre = jnp.moveaxis(grad_act * slope, 0, 1)[None]
    return (grad_pre, grad_weight)


def solution(mesh):
    fine = Mesh(mesh.devices.reshape(4, 4, 2, 4, 2), ("y", "zl", "core", "x", "zh"))
    chan, depth = ("x", "zh"), DEPTH_AXES
    return jax.shard_map(
        work,
        mesh=fine,
        in_specs=(P(None, chan, depth, None), P(None, chan, depth, None), P(None, chan, None)),
        out_specs=(P(None, chan, depth, None), P(None, chan, depth)),
        check_vma=False,
    )
```
